32 devices in a mesh: section: 2 (over y), dp: 16 (over z, x, core).
Axes of the slice: x: 2, y: 2, z: 4, core: 2. Of those that a mesh axis runs over, the one named last changes fastest.
Arguments:
- activations: bfloat16 [2, 8, 256, 3584], P('section', None, 'dp'), may hold values from -8 to 8
- cotangent: bfloat16 [2, 8, 256, 3584], P('section', None, 'dp'), may hold values from -96 to 96
- target_ids: int32 [8, 256], P(None, 'dp'), may hold values from -100 to 152063, as said below
- w_gate: bfloat16 [2, 3584, 96], P('section'), may hold values from -0.09375 to 0.09375
- w_up: bfloat16 [2, 3584, 96], P('section'), may hold values from -0.09375 to 0.09375
- w_down: bfloat16 [2, 96, 3584], P('section'), may hold values from -0.625 to 0.625
Outputs:
- grad_gate: float32 [2, 3584, 96], P('section', 'dp')
- grad_up: float32 [2, 3584, 96], P('section', 'dp')
- grad_down: float32 [2, 96, 3584], P('section', None, 'dp')
- grad_rms: float32 [], replicated
The draws below stay inside these ranges and needn't reach their ends.
Inputs may be any that keep to these rules, and one draw needn't show every extreme that they name: `target_ids`: each entry is -100 (an ignored position) or a token id in 0 to 152063; the share of ignored positions differs between the blocks of 16 tokens of different replicas, from none to about eleven sixteenths.
All inputs are finite; a program needn't handle non-finite values.
Results may differ from the reference program's by a relative error of at most 0.0015.
Values sent between devices are 32-bit elements.
A program may use at most 64 MiB of HBM per device.

```python
import jax
import jax.numpy as jnp
from jax import lax

D = 3584
VOCAB = 152064
HIDDEN_SIZE = 96
MICRO = 8
PIECE_COUNT_PER_REPLICA = 16
TOKENS = 256
LAYERS = 2
N_DP = 16


def draw_target_ids(key, part):
    first_key, second_key, third_key = jax.random.split(key, 3)
    replica_rates = jax.random.randint(first_key, (TOKENS // PIECE_COUNT_PER_REPLICA,), 0, 12)
    column_rate = jnp.repeat(replica_rates, PIECE_COUNT_PER_REPLICA, total_repeat_length=TOKENS)
    dice_rolls = jax.random.randint(second_key, (MICRO, TOKENS), 0, 16)
    token_ids = jax.random.randint(third_key, (MICRO, TOKENS), 0, VOCAB)
    return jnp.where(dice_rolls < column_rate[None, :], -100, token_ids).astype(jnp.int32)


def raised(values, stream_key, source, target, shards_of, factor):
    def block_of(position):
        return (jnp.arange(values.shape[position]) // (values.shape[position] // shards_of)).reshape((-1,) + (1,) * (values.ndim - 1 - position))

    near = jax.random.permutation(stream_key, shards_of)[block_of(target)]
    far = (block_of(target) + shards_of // 2) % shards_of
    return jnp.where((block_of(source) == near) | (block_of(source) == far), factor * values, values)


def steps_of(own_key, extent, pieces, low, largest):
    factor_of, own = 1.0, jax.random.fold_in(own_key, 6)
    for axis_at, parts in pieces:
        heights = jnp.exp(jax.random.uniform(jax.random.fold_in(own, axis_at), (parts,), jnp.float32, low / len(pieces), largest / len(pieces)))
        factor_of = factor_of * jnp.repeat(heights, extent[axis_at] // parts).reshape([-1 if axis == axis_at else 1 for axis in range(len(extent))])
    return factor_of


def normal_values(rng, extent, scale, reach, pieces=(), dtype=jnp.bfloat16):
    array = jax.random.normal(rng, extent, jnp.float32) * scale
    if len(pieces) > 0:
        array = steps_of(rng, extent, pieces, -0.22, 0.18) * array
    return jnp.clip(array, min=-reach, max=reach).astype(dtype)


def noise_with(rng, shape, width, most, cuts, heavy, held_as=jnp.bfloat16):
    values = width * jax.random.normal(rng, shape, jnp.float32)
    if cuts:
        values = values * steps_of(rng, shape, cuts, -0.22, 0.18)
    return jnp.clip(raised(values, jax.random.fold_in(rng, 3), *heavy), -most, most).astype(held_as)


def setup_inputs(seed: int = 0) -> dict:
    arg_keys = jax.random.split(jax.random.key(seed), 7)
    return {
        "activations": noise_with(arg_keys[0], (LAYERS, MICRO, TOKENS, D), 1.0, 8.0, ((0, 2), (2, 16)), (2, 3, 16, 2.0)),
        "cotangent": normal_values(arg_keys[1], (LAYERS, MICRO, TOKENS, D), 16.0, 96.0, ((0, 2), (2, 16))),
        "target_ids": draw_target_ids(jax.random.fold_in(arg_keys[6], 71), 0),
        "w_gate": normal_values(arg_keys[3], (LAYERS, D, HIDDEN_SIZE), D ** -0.5, 0.09375, ((0, 2),)),
        "w_up": normal_values(arg_keys[4], (LAYERS, D, HIDDEN_SIZE), D ** -0.5, 0.09375, ((0, 2),)),
        "w_down": normal_values(arg_keys[5], (LAYERS, HIDDEN_SIZE, D), HIDDEN_SIZE ** -0.5, 0.625, ((0, 2),)),
    }


def finalize_totals(product):
    rounded = lax.optimization_barrier(product.astype(jnp.bfloat16))
    return lax.optimization_barrier(jnp.sum(rounded.astype(jnp.float32), axis=0))

def replica_grads(inputs, upstream, w_gate, w_up, w_down):
    upper_bound = lax.Precision.HIGHEST
    inputs_wide = inputs.astype(jnp.float32)
    incoming_gradient_broad = upstream.astype(jnp.float32)
    gate = jnp.einsum('mtd,dh->mth', inputs_wide, w_gate.astype(jnp.float32), precision=upper_bound)
    up = jnp.einsum('mtd,dh->mth', inputs_wide, w_up.astype(jnp.float32), precision=upper_bound)
    sigmoid_gate = jax.nn.sigmoid(gate)
    activated = gate * sigmoid_gate
    inner_activation = (activated * up).astype(jnp.bfloat16).astype(jnp.float32)
    hidden_grad = jnp.einsum('mtd,hd->mth', incoming_gradient_broad, w_down.astype(jnp.float32), precision=upper_bound)
    gate_grad = (hidden_grad * up * sigmoid_gate * (1.0 + gate * (1.0 - sigmoid_gate))).astype(jnp.bfloat16).astype(jnp.float32)
    up_grad = (hidden_grad * activated).astype(jnp.bfloat16).astype(jnp.float32)
    part_gate = finalize_totals(jnp.einsum('mtd,mth->mdh', inputs_wide, gate_grad, precision=upper_bound))
    part_up = finalize_totals(jnp.einsum('mtd,mth->mdh', inputs_wide, up_grad, precision=upper_bound))
    partial_lowering_weight = finalize_totals(jnp.einsum('flp,flo->fpo', inner_activation, incoming_gradient_broad, precision=upper_bound))
    return (part_gate, part_up, partial_lowering_weight)

def reference(activations, cotangent, target_ids, w_gate, w_up, w_down):
    valid = target_ids >= 0
    count = jnp.sum(valid.astype(jnp.float32))
    mask = valid.astype(jnp.bfloat16)
    gate_list, raising_weight_sequence, down_list = ([], [], [])
    for layer in range(LAYERS):
        inputs = activations[layer].reshape(MICRO, N_DP, PIECE_COUNT_PER_REPLICA, D).transpose(1, 0, 2, 3)
        upstream = (cotangent[layer] * mask[:, :, None]).reshape(MICRO, N_DP, PIECE_COUNT_PER_REPLICA, D).transpose(1, 0, 2, 3)

        def accumulate(carry, pair, layer=layer):
            fresh = replica_grads(pair[0], pair[1], w_gate[layer], w_up[layer], w_down[layer])
            return ((carry[0] + fresh[0], carry[1] + fresh[1], carry[2] + fresh[2]), None)
        start = (jnp.zeros((D, HIDDEN_SIZE), jnp.float32), jnp.zeros((D, HIDDEN_SIZE), jnp.float32), jnp.zeros((HIDDEN_SIZE, D), jnp.float32))
        totals, _ = lax.scan(accumulate, start, (inputs, upstream))
        gate_list.append(totals[0] / count)
        raising_weight_sequence.append(totals[1] / count)
        down_list.append(totals[2] / count)
    grad_gate = jnp.stack(gate_list)
    grad_up = jnp.stack(raising_weight_sequence)
    grad_down = jnp.stack(down_list)
    squares = jnp.sum(grad_gate * grad_gate) + jnp.sum(grad_up * grad_up) + jnp.sum(grad_down * grad_down)
    entries = jnp.float32(LAYERS * 3 * D * HIDDEN_SIZE)
    grad_rms = jnp.sqrt(squares / entries)
    return (grad_gate, grad_up, grad_down, grad_rms)
```

```python
import functools

import jax
import jax.numpy as jnp
from jax import lax
from jax.experimental import pallas as pl
from jax.experimental.pallas import tpu as pltpu
from jax.sharding import PartitionSpec as P

MESH = pl.DeviceIdType.MESH
LANES = 128
PIECES = 3


def line_order(line):
    return [sorted(range(line), key=lambda to: (-abs(to - at), -abs(2 * to - line + 1), to)) for at in range(line)]


def looked_up(table, at, step):
    picked = jnp.int32(0)
    for row, entries in enumerate(table):
        for column, entry in enumerate(entries):
            picked = jnp.where((at == row) & (step == column), jnp.int32(entry), picked)
    return picked


def lane_window(tiles, offset, count):
    first, shift = offset // LANES, offset % LANES
    if shift == 0:
        return tiles[first : first + count]
    lane = lax.broadcasted_iota(jnp.int32, tiles[0].shape, 1)
    turned = [pltpu.roll(tile, LANES - shift, 1) for tile in tiles[first : first + count + 1]]
    turned = turned + [turned[-1]]
    return [jnp.where(lane < LANES - shift, turned[i], turned[i + 1]) for i in range(count)]


def kernel(
    line, entries,
    ids_ref, acts_ref, cot_ref, wg_ref, wu_ref, wd_ref,
    out_ref, rms_ref,
    masked, stage, pair_in, x_out, x_in, total, z_in, full, counts, squares, row_count, row_square,
    pair_send, pair_recv, x_send, x_recv, z_send, z_recv, full_send, full_recv,
    count_send, count_recv, square_send, square_recv,
):
    section, me = lax.axis_index("section"), lax.axis_index("dp")
    sections, replicas = lax.axis_size("section"), lax.axis_size("dp")
    everyone = sections * replicas
    mine = section * replicas + me
    core, x, z = me % 2, (me // 2) % 2, me // 4
    micro, tokens = ids_ref.shape
    columns = micro * tokens
    width = wg_ref.shape[1]
    rows = 3 * width
    half = stage.shape[1] // 2
    piece = half // PIECES
    tiles = acts_ref.shape[1] // line // LANES
    whole = tiles // 2
    order = line_order(line)
    pair = (section, me + 1 - 2 * core)
    across = (section, me + 2 - 4 * x)

    barrier = pltpu.get_barrier_semaphore()

    def greet(step, carry):
        other = (mine + step) % everyone
        pl.semaphore_signal(barrier, inc=1, device_id=(other // replicas, other % replicas), device_id_type=MESH)
        return carry

    lax.fori_loop(1, everyone, greet, 0)

    valid = (ids_ref[...] >= 0).astype(jnp.float32)
    spread = (
        lax.broadcasted_iota(jnp.int32, (tokens, columns), 1) % tokens
        == lax.broadcasted_iota(jnp.int32, (tokens, columns), 0)
    ).astype(jnp.float32)
    own_micro = (
        lax.broadcasted_iota(jnp.int32, (micro, columns), 1) // tokens
        == lax.broadcasted_iota(jnp.int32, (micro, columns), 0)
    )
    laid = jnp.dot(valid, spread, preferred_element_type=jnp.float32)
    mask = jnp.where(own_micro, laid, 0.0)
    row_count[...] = jnp.full(row_count.shape, jnp.sum(mask), jnp.float32)
    counts[me] = row_count[...]

    acts = acts_ref[...]
    gate = jnp.dot(acts, wg_ref[...], preferred_element_type=jnp.float32)
    up = jnp.dot(acts, wu_ref[...], preferred_element_type=jnp.float32)
    hidden_grad = lax.dot_general(
        cot_ref[...], wd_ref[...], (((1,), (1,)), ((), ())), preferred_element_type=jnp.float32
    )
    sig = jax.nn.sigmoid(gate)
    activated = gate * sig
    hidden = activated * up
    gate_grad = hidden_grad * up * sig * (1.0 + gate * (1.0 - sig))
    up_grad = hidden_grad * activated
    for block, values in enumerate((gate_grad, up_grad, hidden)):
        turned = jnp.transpose(values)
        for m in range(micro):
            masked[block, m * width : (m + 1) * width, :] = (turned * mask[m : m + 1, :]).astype(jnp.bfloat16)

    pl.semaphore_wait(barrier, everyone - 1)

    def count_copy(step):
        to = (me + step) % replicas
        return pltpu.make_async_remote_copy(
            src_ref=row_count, dst_ref=counts.at[me], send_sem=count_send.at[step],
            recv_sem=count_recv.at[step], device_id=(section, to), device_id_type=MESH,
        )

    def send_count(step, carry):
        count_copy(step).start()
        return carry

    lax.fori_loop(1, replicas, send_count, 0)

    def pair_copy(k):
        return pltpu.make_async_remote_copy(
            src_ref=stage.at[k, pl.ds(pl.multiple_of((1 - core) * half, 8), half)], dst_ref=pair_in.at[k],
            send_sem=pair_send.at[k], recv_sem=pair_recv.at[k], device_id=pair, device_id_type=MESH,
        )

    def x_copy(k, s):
        return pltpu.make_async_remote_copy(
            src_ref=x_out.at[k, pl.ds(s * piece, piece)], dst_ref=x_in.at[k, pl.ds(s * piece, piece)],
            send_sem=x_send.at[k, s], recv_sem=x_recv.at[k, s], device_id=across, device_id_type=MESH,
        )

    def z_copy(k, s, way, to):
        step = 1 - 2 * way
        return pltpu.make_async_remote_copy(
            src_ref=total.at[k, pl.ds(s * piece, piece)], dst_ref=z_in.at[way, to, pl.ds(s * piece, piece)],
            send_sem=z_send.at[k, s], recv_sem=z_recv.at[way, to, s],
            device_id=(section, me + 4 * step), device_id_type=MESH,
        )

    lane = lax.broadcasted_iota(jnp.int32, (rows // 2, LANES), 1)

    def compute(k):
        to = looked_up(order, z, k % line)
        side = jnp.where(k < line, 1 - x, x)
        start = pl.multiple_of((to * tiles + side * (whole + 1)) * LANES, LANES)
        middle = pl.multiple_of((to * tiles + whole) * LANES, LANES)
        shared = []
        for block in range(3):
            ref = cot_ref if block == 2 else acts_ref
            taken = jnp.concatenate([ref[:, pl.ds(start, whole * LANES)], ref[:, pl.ds(middle, LANES)]], axis=1)
            product = jnp.dot(masked[block], taken, preferred_element_type=jnp.float32)
            rounded = product.astype(jnp.bfloat16).astype(jnp.float32)
            summed = rounded[:width]
            for m in range(1, micro):
                summed = summed + rounded[m * width : (m + 1) * width]
            for j in range(whole):
                stage[k, j * rows + block * width : j * rows + (block + 1) * width, :] = summed[:, j * LANES : (j + 1) * LANES]
            shared.append(summed[:, whole * LANES :])
        shared = jnp.concatenate(shared, axis=0)
        upper, lower = shared[: rows // 2], shared[rows // 2 :]
        near = jnp.where(side == 0, upper, pltpu.roll(upper, LANES // 2, 1))
        far = jnp.where(side == 0, pltpu.roll(lower, LANES // 2, 1), lower)
        stage[k, whole * rows : whole * rows + rows // 2, :] = jnp.where(lane < LANES // 2, near, far)
        pair_copy(k).start()

    def merge(k):
        pair_copy(k).wait_recv()
        value = stage[k, pl.ds(pl.multiple_of(core * half, 8), half)] + pair_in[k]

        @pl.when(k < line)
        def _():
            x_out[k] = value
            for s in range(PIECES):
                x_copy(k, s).start()

        @pl.when(k >= line)
        def _():
            total[k - line] = value

    def chunk(k, carry):
        @pl.when(k < 2 * line)
        def _():
            compute(k)

        @pl.when(k >= 1)
        def _():
            merge(k - 1)

        return carry

    lax.fori_loop(0, 2 * line + 1, chunk, 0)

    def wait_count(step, carry):
        count_copy(step).wait_recv()
        return carry

    def pass_on(k, carry):
        to = looked_up(order, z, k)
        up_way = to > z
        way = jnp.where(up_way, 0, 1)
        behind = jnp.where(up_way, z > 0, z < line - 1)
        for s in range(PIECES):
            at = pl.ds(s * piece, piece)
            x_copy(k, s).wait_recv()
            total[k, at] = total[k, at] + x_in[k, at]

            @pl.when(behind)
            def _():
                z_copy(k, s, way, to).wait_recv()
                total[k, at] = total[k, at] + z_in[way, to, at]

            z_copy(k, s, way, to).start()
        return carry

    lax.fori_loop(0, line - 1, pass_on, 0)
    lax.fori_loop(1, replicas, wait_count, 0)
    count = counts[0]
    for r in range(1, replicas):
        count = count + counts[r]
    inverse = count[0:1]

    def full_copy(s):
        at = pl.ds(pl.multiple_of(core * half + s * piece, 8), piece)
        return pltpu.make_async_remote_copy(
            src_ref=full.at[at], dst_ref=full.at[at], send_sem=full_send.at[s], recv_sem=full_recv.at[s],
            device_id=pair, device_id_type=MESH,
        )

    last = line - 1
    square = jnp.zeros((8, LANES), jnp.float32)
    for s in range(PIECES):
        at = pl.ds(s * piece, piece)
        x_copy(last, s).wait_recv()
        total[last, at] = total[last, at] + x_in[last, at]
        for way in range(2):
            @pl.when((z > 0) if way == 0 else (z < line - 1))
            def _(way=way):
                z_copy(last, s, way, z).wait_recv()
                total[last, at] = total[last, at] + z_in[way, z, at]

        scaled = total[last, at] / inverse
        full[pl.ds(pl.multiple_of(core * half + s * piece, 8), piece)] = scaled
        full_copy(s).start()
        square = square + jnp.sum((scaled * scaled).reshape(piece // 8, 8, LANES), axis=0)
    row_square[...] = square
    squares[mine] = square

    def square_copy(step):
        to = (mine + step) % everyone
        return pltpu.make_async_remote_copy(
            src_ref=row_square, dst_ref=squares.at[mine], send_sem=square_send.at[step],
            recv_sem=square_recv.at[step], device_id=(to // replicas, to % replicas), device_id_type=MESH,
        )

    def send_square(step, carry):
        square_copy(step).start()
        return carry

    lax.fori_loop(1, everyone, send_square, 0)

    for s in range(PIECES):
        full_copy(s).wait_recv()
    packed = full[whole * rows : whole * rows + rows // 2, :]
    rolled = pltpu.roll(packed, LANES // 2, 1)
    shared = jnp.concatenate([jnp.where(x == 0, packed, rolled), jnp.where(x == 0, rolled, packed)], axis=0)
    main = [full[j * rows : (j + 1) * rows, :] for j in range(whole)]
    span = tiles * LANES // 4
    for side in range(2):
        laid_out = main + [shared] if side == 0 else [shared] + main
        for which in range(2):
            @pl.when((x == side) & (core == which))
            def _(laid_out=laid_out, side=side, which=which):
                window = lane_window(laid_out, side * (LANES // 2) + which * span, out_ref.shape[1] // LANES)
                for i, tile in enumerate(window):
                    out_ref[:, i * LANES : (i + 1) * LANES] = tile

    def wait_rest(k, carry):
        pair_copy(k).wait_send()
        return carry

    lax.fori_loop(0, 2 * line, wait_rest, 0)
    for s in range(PIECES):
        full_copy(s).wait_send()
        for k in range(line):
            x_copy(k, s).wait_send()
        for k in range(line - 1):
            z_copy(k, s, jnp.where(z > 0, 1, 0), z).wait_send()

    def wait_sent_count(step, carry):
        count_copy(step).wait_send()
        return carry

    lax.fori_loop(1, replicas, wait_sent_count, 0)

    def wait_squares(step, carry):
        square_copy(step).wait()
        return carry

    lax.fori_loop(1, everyone, wait_squares, 0)
    total_square = squares[0]
    for r in range(1, everyone):
        total_square = total_square + squares[r]
    summed_square = jnp.sum(jnp.sum(total_square, axis=1, keepdims=True), axis=0, keepdims=True)
    rms_ref[...] = jnp.broadcast_to(jnp.sqrt(summed_square / entries), rms_ref.shape)


def fused(line, activations, cotangent, target_ids, w_gate, w_up, w_down):
    _, micro, tokens, model = activations.shape
    width = w_gate.shape[2]
    sections, replicas = lax.axis_size("section"), lax.axis_size("dp")
    rows = 3 * width
    span = model // replicas
    lanes = -(-span // LANES) * LANES
    packed = rows * (model // line // 2) // LANES
    half = packed // 2
    entries = float(sections * rows * model)
    vmem = pl.BlockSpec(memory_space=pltpu.VMEM)
    f32, dma = jnp.float32, pltpu.SemaphoreType.DMA
    out, rms = pl.pallas_call(
        functools.partial(kernel, line, entries),
        out_shape=(jax.ShapeDtypeStruct((rows, lanes), f32), jax.ShapeDtypeStruct((8, LANES), f32)),
        in_specs=[vmem] * 6,
        out_specs=(vmem, vmem),
        scratch_shapes=[
            pltpu.VMEM((3, micro * width, micro * tokens), jnp.bfloat16),
            pltpu.VMEM((2 * line, packed, LANES), f32),
            pltpu.VMEM((2 * line, half, LANES), f32),
            pltpu.VMEM((line, half, LANES), f32),
            pltpu.VMEM((line, half, LANES), f32),
            pltpu.VMEM((line, half, LANES), f32),
            pltpu.VMEM((2, line, half, LANES), f32),
            pltpu.VMEM((packed, LANES), f32),
            pltpu.VMEM((replicas, 8, LANES), f32),
            pltpu.VMEM((sections * replicas, 8, LANES), f32),
            pltpu.VMEM((8, LANES), f32),
            pltpu.VMEM((8, LANES), f32),
            dma((2 * line,)), dma((2 * line,)),
            dma((line, PIECES)), dma((line, PIECES)),
            dma((line, PIECES)), dma((2, line, PIECES)),
            dma((PIECES,)), dma((PIECES,)),
            dma((replicas,)), dma((replicas,)),
            dma((sections * replicas,)), dma((sections * replicas,)),
        ],
        compiler_params=pltpu.CompilerParams(
            collective_id=0, has_side_effects=True, vmem_limit_bytes=48 * 1024 * 1024
        ),
    )(
        target_ids,
        activations[0].reshape(micro * tokens, model),
        cotangent[0].reshape(micro * tokens, model),
        w_gate[0], w_up[0], w_down[0],
    )
    grad_gate = jnp.transpose(out[:width, :span])[None]
    grad_up = jnp.transpose(out[width : 2 * width, :span])[None]
    grad_down = out[2 * width :, :span][None]
    return (grad_gate, grad_up, grad_down, rms[0, 0])


def own_rows(product, span, axis):
    everything = product(jnp.int32(0), lax.axis_size(axis) * span)
    own = lax.psum_scatter(everything, axis, scatter_dimension=0, tiled=True)
    return own


def finalize_totals(product):
    rounded = lax.optimization_barrier(product.astype(jnp.bfloat16))
    return jnp.sum(rounded.astype(jnp.float32), axis=0)


def combine_sums(values):
    replica_total = lax.psum(values, "dp")
    return lax.psum(replica_total, "section")


def shards(activations, cotangent, target_ids, w_gate, w_up, w_down):
    inputs_local = activations[0]
    valid = target_ids >= 0
    local_count = jnp.sum(valid.astype(jnp.float32))
    upstream = cotangent[0] * valid.astype(jnp.bfloat16)[:, :, None]
    gate_weight = w_gate[0]
    up_weight = w_up[0]
    down_weight = w_down[0]
    width = gate_weight.shape[1]
    model_width = inputs_local.shape[2]
    count = lax.psum(local_count, "dp")
    gate = jnp.einsum("mtd,dh->mth", inputs_local, gate_weight, preferred_element_type=jnp.float32)
    up = jnp.einsum("mtd,dh->mth", inputs_local, up_weight, preferred_element_type=jnp.float32)
    sigmoid_gate = jax.nn.sigmoid(gate)
    activated = gate * sigmoid_gate
    inner_activation = (activated * up).astype(jnp.bfloat16)
    hidden_grad = jnp.einsum(
        "mtd,hd->mth", upstream, down_weight, preferred_element_type=jnp.float32
    )
    gate_grad = (hidden_grad * up * sigmoid_gate * (1.0 + gate * (1.0 - sigmoid_gate))).astype(
        jnp.bfloat16
    )
    up_grad = (hidden_grad * activated).astype(jnp.bfloat16)

    def block_terms(start, count_rows):
        input_rows = lax.dynamic_slice_in_dim(inputs_local, start, count_rows, 2)
        incoming_gradient_lines = lax.dynamic_slice_in_dim(upstream, start, count_rows, 2)
        part_gate = finalize_totals(
            jnp.einsum("mtc,mth->mch", input_rows, gate_grad, preferred_element_type=jnp.float32)
        )
        part_up = finalize_totals(
            jnp.einsum("mtc,mth->mch", input_rows, up_grad, preferred_element_type=jnp.float32)
        )
        partial_lowering_weight = finalize_totals(
            jnp.einsum(
                "mth,mtc->mch",
                inner_activation,
                incoming_gradient_lines,
                preferred_element_type=jnp.float32,
            )
        )
        return jnp.concatenate([part_gate, part_up, partial_lowering_weight], axis=1)

    summed = own_rows(block_terms, model_width // lax.axis_size("dp"), "dp")
    entries = jnp.float32(lax.axis_size("section") * 3 * model_width * width)
    scaled = summed / count
    squares = jnp.sum(scaled * scaled)
    totals = combine_sums(squares[None])
    grad_rms = jnp.sqrt(totals[0] / entries)
    grad_gate = scaled[:, :width][None]
    grad_up = scaled[:, width : 2 * width][None]
    grad_down = jnp.transpose(scaled[:, 2 * width :])[None]
    return (grad_gate, grad_up, grad_down, grad_rms)


def line_length(mesh, model, width):
    replicas = mesh.shape["dp"]
    line = replicas // 4
    if replicas % 4 or line < 2 or mesh.shape["section"] != 2:
        return None
    if model % (line * LANES) or (model // line // LANES) % 2 == 0:
        return None
    packed = 3 * width * (model // line // 2)
    return line if packed % (2 * PIECES * 8 * LANES) == 0 else None


def solution(mesh):
    in_specs = (
        P("section", None, "dp", None),
        P("section", None, "dp", None),
        P(None, "dp"),
        P("section", None, None),
        P("section", None, None),
        P("section", None, None),
    )
    out_specs = (P("section", "dp", None), P("section", "dp", None), P("section", None, "dp"), P())

    def program(*arrays):
        line = line_length(mesh, arrays[3].shape[1], arrays[3].shape[2])
        body = shards if line is None else functools.partial(fused, line)
        return jax.shard_map(body, mesh=mesh, in_specs=in_specs, out_specs=out_specs, check_vma=False)(*arrays)

    return program
```
